32 devices in a mesh: groups: 2 (over y), patch: 2 (over x), cfg: 2 (over core), head: 4 (over z).
Axes of the slice: x: 2, y: 2, z: 4, core: 2. Of those that a mesh axis runs over, the one named last changes fastest.
Arguments:
- img_hidden: bfloat16 [2, 1024, 3072], P('cfg', ('groups', 'patch')), parts along dimension 1, may hold values from -40 to 40
- txt_hidden: bfloat16 [2, 64, 3072], P('cfg', ('groups', 'patch')), parts along dimension 1, may hold values from -6 to 6
- modulation: float32 [4, 3, 3072], P(('groups', 'cfg')), parts along dimension 0, may hold values from -4 to 4
- w_qkv: bfloat16 [3072, 3, 1536], P(None, None, 'head'), may hold values from -0.109375 to 0.109375
- q_gain: float32 [128], replicated, may hold values from 1.2 to 2.5
- k_gain: float32 [128], replicated, may hold values from 1.2 to 2.5
- w_out: bfloat16 [1536, 3072], P('head'), may hold values from -0.15625 to 0.15625
- b_out: float32 [3072], replicated, may hold values from -3 to 3
- stale_kv: bfloat16 [2, 2, 1088, 1536], P('cfg', None, ('groups', 'patch'), 'head'), parts along dimension 2, may hold values from -500 to 500
- final_mod: float32 [4, 2, 3072], P(('groups', 'cfg')), parts along dimension 0, may hold values from -3 to 3
- w_final: bfloat16 [3072, 64], replicated, may hold values from -0.109375 to 0.109375
- b_final: float32 [64], replicated, may hold values from -3 to 3
- latent: float32 [1024, 64], P(('groups', 'patch', 'cfg', 'head')), parts along dimension 0, may hold values from -6 to 6
- prev_denoised: float32 [1024, 64], P(('groups', 'patch', 'cfg', 'head')), parts along dimension 0, may hold values from -24 to 24
- guidance: float32 [2], P('groups'), parts along dimension 0, may hold values from 2 to 5
- step_index: int32 [1], replicated, may hold values from 14 to 21
- step_count: int32 [1], replicated, may hold values from 24 to 27
Outputs:
- fresh_kv: bfloat16 [2, 2, 1088, 1536], P('cfg', None, ('groups', 'patch'), 'head'), parts along dimension 2
- next_latent: float32 [1024, 64], P(('groups', 'patch', 'cfg', 'head')), parts along dimension 0
- denoised: float32 [1024, 64], P(('groups', 'patch', 'cfg', 'head')), parts along dimension 0
The draws below stay inside these ranges and needn't reach their ends.
There are 2 independent parts, one for each index of `groups`. The reference program is written for one: setup_inputs(seed, part) draws one part's arguments, and reference() takes and returns one part's arrays. A program takes and returns all parts, laid end to end along the dimension named above; an argument that names none is the same for every part. Nothing has to cross between parts.
All inputs are finite; a program needn't handle non-finite values.
Results may differ from the reference program's by a relative error of at most 0.0075.
The reference program's roundings to bfloat16 on the way (of `weights`, `attn` and `final_in`) count: a program that leaves them out, or rounds other values in their place, can miss the bound.
Values may be sent and summed in bfloat16 or wider, within the bound.
A program may use at most 128 MiB of HBM per device.

```python
import math
import jax
import jax.numpy as jnp
from jax import lax

D = 3072
HD = 128
CH = 64
HEADS = 12
GRID_W = 128
IMG_DEV = 256
TXT_DEV = 16
IMG = 512
TXT = 32
KV_DEV = 272
KVTOK = 544
N_PATCH = 2


def draw_img_hidden(key, part):
    key_base = jax.random.fold_in(key, 0)
    values = jax.random.normal(key_base, (2, IMG, D), jnp.float32)
    return jnp.clip(values, -40.0, 40.0).astype(jnp.bfloat16)


def draw_stale_kv(key, part):
    key_base = jax.random.fold_in(key, 0)
    width = HEADS * HD
    values = jax.random.normal(key_base, (2, 2, KVTOK, width), jnp.float32)
    values = values * jnp.array([1.5, 1.0], jnp.float32).reshape(1, 2, 1, 1)
    return jnp.clip(values, -500.0, 500.0).astype(jnp.bfloat16)


def shard_levels(stream_key, shape, cuts, low, high):
    def one(axis_at, shards_of):
        steps = jax.random.uniform(jax.random.fold_in(jax.random.fold_in(stream_key, 6), axis_at), (shards_of,), jnp.float32, low / len(cuts), high / len(cuts))
        return jnp.repeat(jnp.exp(steps), shape[axis_at] // shards_of).reshape((-1,) + (1,) * (len(shape) - axis_at - 1))

    loudness = one(*cuts[0])
    for cut in cuts[1:]:
        loudness = loudness * one(*cut)
    return loudness


def normal_values(rng, extent, deviation, limit, shards=(), held_as=jnp.bfloat16):
    drawn = deviation * jax.random.normal(rng, extent, jnp.float32)
    if shards:
        drawn = drawn * shard_levels(rng, extent, shards, -0.22, 0.18)
    return jnp.clip(drawn, -limit, limit).astype(held_as)


def setup_inputs(seed: int = 0, part: int = 0) -> dict:
    splits = jax.random.split(jax.random.key(seed), 18)
    part_splits = jax.random.split(jax.random.fold_in(splits[17], part), 18)
    img_hidden = draw_img_hidden(jax.random.fold_in(jax.random.fold_in(splits[17], part), 71), part)
    txt_hidden = normal_values(part_splits[1], (2, TXT, D), 1.0, 6.0, ((0, 2), (1, 2)))
    modulation = normal_values(part_splits[2], (2, 3, D), 0.7, 4.0, ((0, 2),), jnp.float32)
    w_qkv = normal_values(splits[3], (D, 3, HEADS * HD), D ** -0.5, 0.109375, ((2, 4),))
    q_gain = jnp.clip(jnp.exp(jax.random.uniform(splits[4], (HD,), jnp.float32, math.log(1.2), math.log(2.5))), 1.2, 2.5)
    k_gain = jnp.clip(jnp.exp(jax.random.uniform(splits[5], (HD,), jnp.float32, math.log(1.2), math.log(2.5))), 1.2, 2.5)
    w_out = normal_values(splits[6], (HEADS * HD, D), (HEADS * HD) ** -0.5, 0.15625, ((0, 4),))
    b_out = normal_values(splits[7], (D,), 0.5, 3.0, (), jnp.float32)
    stale_kv = draw_stale_kv(jax.random.fold_in(jax.random.fold_in(splits[17], part), 71), part)
    final_mod = normal_values(part_splits[9], (2, 2, D), 0.5, 3.0, ((0, 2),), jnp.float32)
    w_final = normal_values(splits[10], (D, CH), D ** -0.5, 0.109375)
    b_final = normal_values(splits[11], (CH,), 0.5, 3.0, (), jnp.float32)
    latent = normal_values(part_splits[12], (IMG, CH), 1.0, 6.0, ((0, 16),), jnp.float32)
    prev_denoised = normal_values(part_splits[13], (IMG, CH), 4.0, 24.0, ((0, 16),), jnp.float32)
    guidance = jnp.clip(jax.random.uniform(part_splits[14], (1,), jnp.float32, 2.0, 5.0), 2.0, 5.0)
    step_index = jax.random.randint(splits[15], (1,), 14, 22).astype(jnp.int32)
    step_count = jax.random.randint(splits[16], (1,), 24, 28).astype(jnp.int32)
    return dict(img_hidden=img_hidden, txt_hidden=txt_hidden, modulation=modulation, w_qkv=w_qkv, q_gain=q_gain, k_gain=k_gain, w_out=w_out, b_out=b_out, stale_kv=stale_kv, final_mod=final_mod, w_final=w_final, b_final=b_final, latent=latent, prev_denoised=prev_denoised, guidance=guidance, step_index=step_index, step_count=step_count)


epsilon = 1e-06
time_shift = 3.0

def layer_norm(values):
    mean_val = lax.optimization_barrier(jnp.mean(values, axis=-1, keepdims=True))
    centered = values - mean_val
    variance = lax.optimization_barrier(jnp.mean(centered * centered, axis=-1, keepdims=True))
    return centered * lax.rsqrt(variance + epsilon)

def rms_norm(values, gain_vec):
    return values * lax.rsqrt(lax.optimization_barrier(jnp.mean(values * values, axis=-1, keepdims=True)) + epsilon) * gain_vec

def rotate(values, positions, grid_width):
    quarter = values.shape[-1] // 4
    freqs = 10000.0 ** (-jnp.arange(quarter, dtype=jnp.float32) / quarter)
    row_pos = (positions // grid_width).astype(jnp.float32)
    col_pos = (positions % grid_width).astype(jnp.float32)
    angles = jnp.stack([row_pos[:, None] * freqs[None, :], col_pos[:, None] * freqs[None, :]], axis=1)
    cosine = jnp.cos(angles)[:, None]
    sine = jnp.sin(angles)[:, None]
    shaped = values.reshape(values.shape[0], values.shape[1], 2, 2, quarter)
    first = shaped[:, :, :, 0]
    second = shaped[:, :, :, 1]
    turned = jnp.stack([first * cosine - second * sine, second * cosine + first * sine], axis=3)
    return turned.reshape(values.shape)

def noise_level(index, count):
    frac = 1.0 - index / count
    lift = math.exp(time_shift)
    return lift * frac / (lift * frac + 1.0 - frac)

def log_ratio(sigma_val):
    return jnp.log(1.0 - sigma_val) - jnp.log(sigma_val)

def solver_step(cond, uncond, guidance, step_index, step_count, latent, prev_denoised):
    guided = uncond + guidance[0] * (cond - uncond)
    index = step_index[0].astype(jnp.float32)
    count = step_count[0].astype(jnp.float32)
    sigma_prev = noise_level(index - 1.0, count)
    sigma_now = noise_level(index, count)
    sigma_next = noise_level(index + 1.0, count)
    step_now = log_ratio(sigma_next) - log_ratio(sigma_now)
    step_prev = log_ratio(sigma_now) - log_ratio(sigma_prev)
    ratio = step_prev / step_now
    denoised = latent - sigma_now * guided
    blend = (1.0 + 0.5 / ratio) * denoised - 0.5 / ratio * prev_denoised
    next_latent = sigma_next / sigma_now * latent - (1.0 - sigma_next) * (jnp.exp(-step_now) - 1.0) * blend
    return (next_latent, denoised)

def reference(img_hidden, txt_hidden, modulation, w_qkv, q_gain, k_gain, w_out, b_out, stale_kv, final_mod, w_final, b_final, latent, prev_denoised, guidance, step_index, step_count):
    inv_root = HD ** (-0.5)
    head_width = HEADS * HD
    weight_flat = w_qkv.reshape(D, 3 * head_width)
    positions = jnp.arange(IMG, dtype=jnp.int32)
    fresh_list = []
    velocities = []
    for branch in range(2):
        shift_vec = modulation[branch, 0]
        scale_vec = modulation[branch, 1]
        gate_vec = modulation[branch, 2]
        modded_img = (layer_norm(img_hidden[branch].astype(jnp.float32)) * (1.0 + scale_vec) + shift_vec).astype(jnp.bfloat16)
        modded_txt = (layer_norm(txt_hidden[branch].astype(jnp.float32)) * (1.0 + scale_vec) + shift_vec).astype(jnp.bfloat16)
        proj_img = jnp.dot(modded_img, weight_flat, preferred_element_type=jnp.float32).reshape(IMG, 3, HEADS, HD)
        proj_txt = jnp.dot(modded_txt, weight_flat, preferred_element_type=jnp.float32).reshape(TXT, 3, HEADS, HD)
        queries = lax.optimization_barrier(rotate(rms_norm(proj_img[:, 0], q_gain), positions, GRID_W).astype(jnp.bfloat16))
        img_keys = rotate(rms_norm(proj_img[:, 1], k_gain), positions, GRID_W).astype(jnp.bfloat16)
        img_vals = proj_img[:, 2].astype(jnp.bfloat16)
        txt_keys = rms_norm(proj_txt[:, 1], k_gain).astype(jnp.bfloat16)
        txt_vals = proj_txt[:, 2].astype(jnp.bfloat16)

        def joined(txt_part, img_part):
            return jnp.concatenate([txt_part.reshape(N_PATCH, TXT_DEV, HEADS, HD), img_part.reshape(N_PATCH, IMG_DEV, HEADS, HD)], axis=1).reshape(KVTOK, HEADS, HD)
        fresh_keys = lax.optimization_barrier(joined(txt_keys, img_keys))
        fresh_vals = lax.optimization_barrier(joined(txt_vals, img_vals))
        fresh_list.append(jnp.stack([fresh_keys.reshape(KVTOK, head_width), fresh_vals.reshape(KVTOK, head_width)]))
        stale_keys = stale_kv[branch, 0].reshape(KVTOK, HEADS, HD)
        stale_vals = stale_kv[branch, 1].reshape(KVTOK, HEADS, HD)

        def attend(block):
            query_blk = lax.dynamic_slice_in_dim(queries, block * IMG_DEV, IMG_DEV, 0)
            own_keys = lax.dynamic_slice_in_dim(fresh_keys, block * KV_DEV, KV_DEV, 0)
            own_vals = lax.dynamic_slice_in_dim(fresh_vals, block * KV_DEV, KV_DEV, 0)
            keys_all = lax.dynamic_update_slice_in_dim(stale_keys, own_keys, block * KV_DEV, 0)
            vals_all = lax.dynamic_update_slice_in_dim(stale_vals, own_vals, block * KV_DEV, 0)
            scores = jnp.einsum('qhd,khd->hqk', query_blk.astype(jnp.float32), keys_all.astype(jnp.float32)) * inv_root
            top = lax.optimization_barrier(jnp.max(scores, axis=-1, keepdims=True))
            expo = jnp.exp(scores - top)
            denom = lax.optimization_barrier(jnp.sum(expo, axis=-1))
            weights = lax.optimization_barrier(expo.astype(jnp.bfloat16))
            weighted = jnp.einsum('hqk,khd->hqd', weights.astype(jnp.float32), vals_all.astype(jnp.float32))
            attn_blk = weighted / denom[..., None]
            return attn_blk.transpose(1, 0, 2).reshape(IMG_DEV, head_width).astype(jnp.bfloat16)
        attn = lax.map(attend, jnp.arange(N_PATCH, dtype=jnp.int32)).reshape(IMG, head_width)
        projected = jnp.dot(attn, w_out, preferred_element_type=jnp.float32)
        mixed = img_hidden[branch].astype(jnp.float32) + gate_vec * (projected + b_out)
        final_in = (layer_norm(mixed) * (1.0 + final_mod[branch, 1]) + final_mod[branch, 0]).astype(jnp.bfloat16)
        velocities.append(jnp.dot(final_in, w_final, preferred_element_type=jnp.float32) + b_final)
    next_latent, denoised = solver_step(velocities[0], velocities[1], guidance, step_index, step_count, latent, prev_denoised)
    return (jnp.stack(fresh_list), next_latent, denoised)
```

```python
import functools
import math

import jax
import jax.numpy as jnp
from jax import lax
from jax.experimental import pallas as pl
from jax.experimental.pallas import tpu as pltpu
from jax.sharding import PartitionSpec as P

HD = 128
GRID_W = 128
LN_ROWS = 16
LN_UNROLL = 4
THIRDS = 3
PLANE = 8
VMEM_MAIN = 67043328

epsilon = 1e-06
time_shift = 3.0
MESH = pl.DeviceIdType.MESH


def normed(values):
    centered = values - jnp.mean(values, axis=-1, keepdims=True)
    variance = jnp.mean(centered * centered, axis=-1, keepdims=True)
    return centered * lax.rsqrt(variance + epsilon)


def noise_level(index, count):
    frac = 1.0 - index / count
    lift = math.exp(time_shift)
    return lift * frac / (lift * frac + 1.0 - frac)


def log_ratio(sigma_val):
    return jnp.log(1.0 - sigma_val) - jnp.log(sigma_val)


def rotation_tables(cos_ref, sin_ref, txt_rows, first_pos):
    shape = cos_ref.shape
    quarter = HD // 4
    rows = lax.broadcasted_iota(jnp.int32, shape, 0)
    lanes = lax.broadcasted_iota(jnp.int32, shape, 1)
    pos = jnp.where(rows >= txt_rows, rows - txt_rows + first_pos, 0)
    place = jnp.where(lanes < 2 * quarter, pos // GRID_W, pos % GRID_W).astype(jnp.float32)
    step = (lanes % quarter).astype(jnp.float32)
    angle = place * jnp.exp(step * (-math.log(10000.0) / quarter))
    sine = jnp.sin(angle)
    cos_ref[...] = jnp.cos(angle)
    sin_ref[...] = jnp.where(lanes % (2 * quarter) < quarter, -sine, sine)


def rotated(values, gain, cosine, sine):
    quarter = HD // 4
    v = values * lax.rsqrt(jnp.mean(values * values, axis=-1, keepdims=True) + epsilon) * gain
    lanes = lax.broadcasted_iota(jnp.int32, v.shape, 1)
    swapped = jnp.where(
        lanes % (2 * quarter) < quarter,
        pltpu.roll(v, HD - quarter, 1),
        pltpu.roll(v, quarter, 1),
    )
    return (v * cosine + swapped * sine).astype(jnp.bfloat16)


def kernel(
    n_patch,
    hid, txt, mod, w_qkv, q_gain, k_gain, w_out, b_out, stale, fmod, w_fin, b_fin, lat, prev,
    guidance, step_index, step_count,
    fresh_s, step_o,
    hid_v, txt_v, mod_v, w_v, qg_v, kg_v, wo_v, bo_v, fmod_v, wf_v, bf_v, lat_v, prev_v,
    modded, proj, cos_s, sin_s, q_s, kv_s, m_s, l_s, acc_s, attn_s, attn_in,
    w_in, out_acc, hi_s, lo_s, stat_s, vel_s, vel_in, vec_s, vec_in,
    loc_sem, kv_send, kv_recv, wz_send, wz_recv, wx_send, wx_recv, wy_send, wy_recv,
    wc_send, wc_recv, at_send, at_recv, fw_send, v_send, v_recv, u_send, u_recv,
):
    patch = lax.axis_index("patch")
    group = lax.axis_index("groups")
    cfg = lax.axis_index("cfg")
    head = lax.axis_index("head")
    side = lax.div(head, 2)
    third = lax.rem(head, THIRDS)
    is_end = third == 0
    is_mid = third != 0
    mate = 2 * side + 1 - lax.rem(head, 2)
    partners = (mate, 3 - head, lax.rem(head + 2, 4))
    x_bit = lax.rem(patch, 2)
    x_dev = {"patch": patch + 1 - 2 * x_bit}
    y_dev = {"groups": 1 - group}
    c_dev = {"cfg": 1 - cfg}
    img_rows, d = hid_v.shape
    txt_rows = txt_v.shape[0]
    head_width = wo_v.shape[0]
    heads = head_width // HD
    out_rows = lat_v.shape[0]
    half = img_rows // 2
    cols = d // THIRDS
    share = head_width // PLANE
    my_cols = pl.ds(pl.multiple_of(third * cols, HD), cols)
    half_at = pl.ds(pl.multiple_of(side * half, half), half)

    pairs = [
        (mod, mod_v), (txt, txt_v), (hid, hid_v),
        (w_qkv.at[1], w_v.at[1]), (w_qkv.at[2], w_v.at[2]), (w_qkv.at[0], w_v.at[0]),
        (k_gain, kg_v), (q_gain, qg_v), (w_out.at[:, my_cols], wo_v), (b_out, bo_v),
        (fmod, fmod_v), (w_fin.at[:, my_cols], wf_v.at[pl.ds(0, w_fin.shape[0])]),
        (b_fin, bf_v), (lat, lat_v), (prev, prev_v),
    ]
    local = [pltpu.make_async_copy(s, t, loc_sem.at[i]) for i, (s, t) in enumerate(pairs)]
    for copy in local:
        copy.start()

    def remote(source, target, send, recv, device):
        return pltpu.make_async_remote_copy(
            src_ref=source, dst_ref=target, send_sem=send, recv_sem=recv,
            device_id=device, device_id_type=MESH,
        )

    peers = [{"patch": lax.rem(patch + j, n_patch)} for j in range(1, n_patch)] + [y_dev]
    owners = [(dc, dh) for dc in range(2) for dh in range(4)]
    for dc, dh in owners[1:]:
        peers.append({"cfg": lax.rem(cfg + dc, 2), "head": lax.rem(head + dh, 4)})
    barrier = pltpu.get_barrier_semaphore()
    for peer in peers:
        pl.semaphore_signal(barrier, inc=1, device_id=peer, device_id_type=MESH)
    rotation_tables(cos_s, sin_s, txt_rows, patch * img_rows)
    pl.semaphore_wait(barrier, len(peers))

    def kv_copy(j, hh, which):
        return remote(
            stale.at[which, :, pl.ds(hh * HD, HD)], kv_s.at[j - 1, which, hh],
            kv_send.at[j - 1, which, hh], kv_recv.at[j - 1, which, hh],
            {"patch": lax.rem(patch + j, n_patch)},
        )

    for hh in range(heads):
        for which in range(2):
            for j in range(1, n_patch):
                kv_copy(j, hh, which).start()

    def unit(x, y, c):
        one = 1 - cfg if c else cfg
        two = 1 - group if y else group
        three = 1 - x_bit if x else x_bit
        return pl.ds(pl.multiple_of((one * 4 + two * 2 + three) * share, 16), share)

    own = unit(0, 0, 0)

    def w_over_z(r):
        to = partners[r]
        at = pl.ds(pl.multiple_of(lax.rem(to, THIRDS) * cols, HD), cols)
        return remote(
            w_out.at[own, at], w_in.at[r, own], wz_send.at[r], wz_recv.at[r], {"head": to}
        )

    def w_over_x(r):
        at = w_in.at[r, own]
        return remote(at, at, wx_send.at[r], wx_recv.at[r], x_dev)

    def w_over_y(r, k):
        at = w_in.at[r, unit(k, 0, 0)]
        return remote(at, at, wy_send.at[r, k], wy_recv.at[r, k], y_dev)

    def w_over_c(r, k):
        at = w_in.at[r, unit(k % 2, k // 2, 0)]
        return remote(at, at, wc_send.at[r, k], wc_recv.at[r, k], c_dev)

    order = (0, 2, 1)
    for r in order:
        w_over_z(r).start()

    def w_landed(r):
        w_over_z(r).wait_recv()
        w_over_x(r).start()
        w_over_y(r, 0).start()
        w_over_c(r, 0).start()

    for copy in local[:3]:
        copy.wait()

    def modulate(values):
        out = normed(values.astype(jnp.float32)) * (1.0 + mod_v[1]) + mod_v[0]
        return out.astype(jnp.bfloat16)

    modded[pl.ds(0, txt_rows), :] = modulate(txt_v[...])

    def ln_step(i, carry):
        at = pl.multiple_of(i * LN_ROWS, LN_ROWS)
        modded[pl.ds(at + txt_rows, LN_ROWS), :] = modulate(hid_v[pl.ds(at, LN_ROWS), :])
        return carry

    lax.fori_loop(0, img_rows // LN_ROWS, ln_step, 0, unroll=LN_UNROLL)

    local[3].wait()
    local[6].wait()
    proj[...] = jnp.dot(modded[...], w_v[1], preferred_element_type=jnp.float32)
    for hh in range(heads):
        at = pl.ds(hh * HD, HD)
        fresh_s[0, :, at] = rotated(proj[:, at], kg_v[...], cos_s[...], sin_s[...])
    local[4].wait()
    fresh_s[1] = jnp.dot(modded[...], w_v[2], preferred_element_type=jnp.float32).astype(
        jnp.bfloat16
    )
    local[5].wait()
    local[7].wait()
    img_at = pl.ds(txt_rows, img_rows)
    proj[img_at, :] = jnp.dot(modded[img_at, :], w_v[0], preferred_element_type=jnp.float32)
    for hh in range(heads):
        at = pl.ds(hh * HD, HD)
        q_s[:, at] = rotated(proj[img_at, at], qg_v[...], cos_s[img_at, :], sin_s[img_at, :])

    exp_scale = HD ** (-0.5) * math.log2(math.e)

    def scores_of(hh, keys):
        return (
            lax.dot_general(
                q_s[:, pl.ds(hh * HD, HD)],
                keys,
                (((1,), (1,)), ((), ())),
                preferred_element_type=jnp.float32,
            )
            * exp_scale
        )

    for hh in range(heads):
        at = pl.ds(hh * HD, HD)
        scores = scores_of(hh, fresh_s[0, :, at])
        top = jnp.max(scores, axis=-1, keepdims=True)
        expo = jnp.exp2(scores - top)
        m_s[hh] = top
        l_s[hh] = jnp.sum(expo, axis=-1, keepdims=True)
        acc_s[hh] = jnp.dot(
            expo.astype(jnp.bfloat16), fresh_s[1, :, at], preferred_element_type=jnp.float32
        )

    w_landed(order[0])

    def f32(values):
        return values.astype(jnp.float32)

    for copy in local[8:]:
        copy.wait()
    channels = lat_v.shape[1]
    wf_v[pl.ds(channels, wf_v.shape[0] - channels), :] = jnp.zeros(
        (wf_v.shape[0] - channels, cols), jnp.bfloat16
    )
    scale_up = 1.0 + fmod_v[1:2, my_cols]
    shift_up = fmod_v[0:1, my_cols]
    lines = lax.broadcasted_iota(jnp.int32, (8, cols), 0)
    scale_hi, shift_hi = f32(scale_up.astype(jnp.bfloat16)), f32(shift_up.astype(jnp.bfloat16))
    rows_up = jnp.where(lines == 0, scale_hi, jnp.where(lines == 1, scale_up - scale_hi, 0.0))
    rows_up = jnp.where(lines == 2, shift_hi, jnp.where(lines == 3, shift_up - shift_hi, rows_up))

    def to_channels(values):
        return lax.dot_general(
            values, wf_v[...], (((1,), (1,)), ((), ())), preferred_element_type=jnp.float32
        )

    vec_s[...] = to_channels(rows_up.astype(jnp.bfloat16))

    def each_owner(act):
        for dc, dh in owners:
            to_cfg, to_head = lax.rem(cfg + dc, 2), lax.rem(head + dh, 4)
            wanted = is_mid | (to_cfg == side)
            slot = to_cfg * 4 + to_head
            where_to = {"cfg": to_cfg, "head": to_head}
            at = dc * 4 + dh

            @pl.when(wanted)
            def _():
                act(at, slot, where_to, dc == 0 and dh == 0)

    def vec_copy(at, where_to):
        return remote(
            vec_s, vec_in.at[cfg, third], u_send.at[at], u_recv.at[cfg, third], where_to
        )

    def vel_copy(at, slot, where_to):
        return remote(
            vel_s.at[slot], vel_in.at[cfg, third], v_send.at[at], v_recv.at[cfg, third], where_to
        )

    def vec_start(at, slot, where_to, mine):
        if mine:
            vec_in[cfg, third] = vec_s[...]
        else:
            vec_copy(at, where_to).start()

    each_owner(vec_start)

    def attn_full(r, hh):
        return remote(
            attn_s.at[hh], attn_in.at[r, hh], at_send.at[r, hh], at_recv.at[r, hh],
            {"head": partners[r]},
        )

    def attn_half(hh):
        return remote(
            attn_s.at[hh, half_at], attn_in.at[0, hh, half_at], at_send.at[0, hh],
            at_recv.at[0, hh], {"head": mate},
        )

    def attn_relay(r, hh):
        return remote(
            attn_in.at[r, hh, half_at], attn_in.at[3 - r, hh, half_at], fw_send.at[r - 1, hh],
            at_recv.at[3 - r, hh], {"head": mate},
        )

    def other_block(j, hh):
        scores = scores_of(hh, kv_s[j, 0, hh])
        old = m_s[hh]
        top = jnp.maximum(old, jnp.max(scores, axis=-1, keepdims=True))
        factor = jnp.exp2(old - top)
        expo = jnp.exp2(scores - top)
        m_s[hh] = top
        l_s[hh] = l_s[hh] * factor + jnp.sum(expo, axis=-1, keepdims=True)
        acc_s[hh] = acc_s[hh] * factor + jnp.dot(
            expo.astype(jnp.bfloat16), kv_s[j, 1, hh], preferred_element_type=jnp.float32
        )

    for hh in range(heads):
        for j in range(1, n_patch):
            for which in range(2):
                kv_copy(j, hh, which).wait_recv()
        if n_patch <= 2:
            for j in range(n_patch - 1):
                other_block(j, hh)
        else:
            lax.fori_loop(0, n_patch - 1, lambda j, c: (other_block(j, hh), c)[1], 0)
        attn_s[hh] = (acc_s[hh] / l_s[hh]).astype(jnp.bfloat16)

        @pl.when(is_end)
        def _():
            attn_full(2, hh).start()
            attn_full(0, hh).start()

        @pl.when(is_mid)
        def _():
            attn_full(1, hh).start()
            attn_half(hh).start()

        if hh < 2:
            w_landed(order[hh + 1])

    def joined(ref, at):
        return jnp.concatenate([ref[hh, at, :] for hh in range(heads)], axis=1)

    def project(ref, weights, at):
        return jnp.dot(joined(ref, at), weights, preferred_element_type=jnp.float32)

    everything = pl.ds(0, img_rows)

    def on_rows(act):
        @pl.when(is_mid)
        def _():
            act(everything, img_rows)

        @pl.when(is_end)
        def _():
            act(half_at, half)

    def start_acc(at, count):
        out_acc[at, :] = project(attn_s, wo_v[...], at)

    on_rows(start_acc)

    for r in order:
        w_over_y(r, 0).wait_recv()
        w_over_c(r, 2).start()
    for hh, r in enumerate(order):
        w_over_x(r).wait_recv()
        w_over_y(r, 1).start()
        w_over_c(r, 1).start()

        @pl.when(is_mid)
        def _():
            for s in (1, 2):
                attn_full(s, hh).wait_recv()
                attn_relay(s, hh).start()

    for r in order:
        w_over_y(r, 1).wait_recv()
        w_over_c(r, 3).start()

    @pl.when(is_mid)
    def _():
        for hh in range(heads):
            attn_full(0, hh).wait_recv()

    @pl.when(is_end)
    def _():
        for hh in range(heads):
            attn_half(hh).wait_recv()
            for s in (1, 2):
                attn_relay(3 - s, hh).wait_recv()

    for r in order:
        for k in range(4):
            w_over_c(r, k).wait_recv()

        def add_acc(at, count):
            out_acc[at, :] += project(attn_in.at[r], w_in[r], at)

        on_rows(add_acc)

    gate = mod_v[2, :, my_cols]
    bias = bo_v[:, my_cols]
    lanes = lax.broadcasted_iota(jnp.int32, (LN_ROWS, HD), 1)

    def final_step(first):
        def run(i, carry):
            at = pl.ds(pl.multiple_of(first + i * LN_ROWS, LN_ROWS), LN_ROWS)
            mixed = f32(hid_v[at, my_cols]) + gate * (out_acc[at, :] + bias)
            mean = jnp.mean(mixed, axis=-1, keepdims=True)
            centered = mixed - mean
            spread = jnp.sum(centered * centered, axis=-1, keepdims=True)
            scaled = centered * scale_up
            high = scaled.astype(jnp.bfloat16)
            hi_s[at, :] = high
            lo_s[at, :] = (scaled - f32(high)).astype(jnp.bfloat16)
            stat_s[at, :] = jnp.where(
                lanes == channels, mean, jnp.where(lanes == channels + 1, spread, 0.0)
            )
            return carry

        return run

    def finish(at, count):
        first = 0 if count == img_rows else side * half
        lax.fori_loop(0, count // LN_ROWS, final_step(first), 0, unroll=LN_UNROLL)
        value = to_channels(hi_s[at, :]) + to_channels(lo_s[at, :]) + stat_s[at, :]
        for i in range(count // out_rows):
            slot = i if count == img_rows else side * 4 + i
            vel_s[slot] = value[i * out_rows : (i + 1) * out_rows]

    on_rows(finish)

    def vel_start(at, slot, where_to, mine):
        if mine:
            vel_in[cfg, third] = vel_s[slot]
        else:
            vel_copy(at, slot, where_to).start()

    each_owner(vel_start)

    ones = jnp.ones(lat_v.shape, jnp.float32)
    index = ones * step_index[0].astype(jnp.float32)
    count = ones * step_count[0].astype(jnp.float32)
    sigma_prev = noise_level(index - 1.0, count)
    sigma_now = noise_level(index, count)
    sigma_next = noise_level(index + 1.0, count)
    step_now = log_ratio(sigma_next) - log_ratio(sigma_now)
    step_prev = log_ratio(sigma_now) - log_ratio(sigma_prev)
    ratio = step_prev / step_now
    shrink = (1.0 - sigma_next) * (jnp.exp(-step_now) - 1.0)
    latent = lat_v[...]

    for b in range(2):
        for k in range(THIRDS):
            source = 3 * cfg if k == 0 else k

            @pl.when((cfg != b) | (head != source))
            def _():
                where_to = {"cfg": cfg, "head": head}
                for kind in (0, 1):
                    pltpu.make_async_remote_copy(
                        src_ref=vec_s if kind else vel_s.at[0],
                        dst_ref=vec_in.at[b, k] if kind else vel_in.at[b, k],
                        send_sem=u_send.at[0] if kind else v_send.at[0],
                        recv_sem=u_recv.at[b, k] if kind else v_recv.at[b, k],
                        device_id=c_dev,
                        device_id_type=MESH,
                    ).wait_recv()

    def velocity(b):
        means = [vel_in[b, k, :, channels : channels + 1] for k in range(THIRDS)]
        mean = sum(means) / THIRDS
        spread = sum(vel_in[b, k, :, channels + 1 : channels + 2] for k in range(THIRDS))
        spread = spread + cols * sum((m - mean) * (m - mean) for m in means)
        total = 0.0
        base = bf_v[...]
        for k in range(THIRDS):
            lift = vec_in[b, k, 0:1, :channels] + vec_in[b, k, 1:2, :channels]
            base = base + vec_in[b, k, 2:3, :channels] + vec_in[b, k, 3:4, :channels]
            total = total + vel_in[b, k, :, :channels] + (means[k] - mean) * lift
        return total * lax.rsqrt(spread / d + epsilon) + base

    cond, uncond = velocity(0), velocity(1)
    guided = uncond + guidance[0] * (cond - uncond)
    denoised = latent - sigma_now * guided
    blend = (1.0 + 0.5 / ratio) * denoised - 0.5 / ratio * prev_v[...]
    step_o[1] = denoised
    step_o[0] = sigma_next / sigma_now * latent - shrink * blend

    for hh in range(heads):
        for which in range(2):
            for j in range(1, n_patch):
                kv_copy(j, hh, which).wait_send()
    for r in order:
        w_over_z(r).wait_send()
        w_over_x(r).wait_send()
        for k in range(2):
            w_over_y(r, k).wait_send()
        for k in range(4):
            w_over_c(r, k).wait_send()

    @pl.when(is_end)
    def _():
        for hh in range(heads):
            attn_full(0, hh).wait_send()
            attn_full(2, hh).wait_send()

    @pl.when(is_mid)
    def _():
        for hh in range(heads):
            attn_full(1, hh).wait_send()
            attn_half(hh).wait_send()
            for s in (1, 2):
                attn_relay(s, hh).wait_send()

    def sent(at, slot, where_to, mine):
        if not mine:
            vec_copy(at, where_to).wait_send()
            vel_copy(at, slot, where_to).wait_send()

    each_owner(sent)


def deliver(fresh, stepped, fresh_o, next_o, den_o, fresh_v, step_v, in_sem, out_sem):
    loads = [
        pltpu.make_async_copy(stepped, step_v, in_sem.at[0]),
        pltpu.make_async_copy(fresh, fresh_v, in_sem.at[1]),
    ]
    for copy in loads:
        copy.start()
    pairs = ((step_v.at[0], next_o), (step_v.at[1], den_o), (fresh_v, fresh_o))
    stores = [pltpu.make_async_copy(s, t, out_sem.at[i]) for i, (s, t) in enumerate(pairs)]
    loads[0].wait()
    stores[0].start()
    stores[1].start()
    loads[1].wait()
    stores[2].start()
    for copy in stores:
        copy.wait()


def body(
    n_patch,
    img_hidden, txt_hidden, modulation, w_qkv, q_gain, k_gain, w_out, b_out, stale_kv,
    final_mod, w_final, b_final, latent, prev_denoised, guidance, step_index, step_count,
):
    bf16, f32 = jnp.bfloat16, jnp.float32
    img_rows, d = img_hidden.shape[1:]
    txt_rows = txt_hidden.shape[1]
    kv_rows = img_rows + txt_rows
    head_width = w_out.shape[0]
    heads = head_width // HD
    out_rows, channels = latent.shape
    cols = d // THIRDS
    args = (
        img_hidden[0],
        txt_hidden[0],
        modulation.transpose(1, 0, 2),
        w_qkv.transpose(1, 0, 2),
        q_gain[None],
        k_gain[None],
        w_out,
        b_out[None],
        stale_kv[0],
        final_mod[0],
        w_final.T,
        b_final[None],
        latent,
        prev_denoised,
    )
    dma = pltpu.SemaphoreType.DMA
    shapes = {6: (head_width, cols), 10: (HD, cols)}
    remotes = n_patch - 1
    scratch = [
        pltpu.VMEM(shapes.get(i, a.shape), a.dtype) for i, a in enumerate(args) if i != 8
    ] + [
        pltpu.VMEM((kv_rows, d), bf16),
        pltpu.VMEM((kv_rows, head_width), f32),
        pltpu.VMEM((kv_rows, HD), f32),
        pltpu.VMEM((kv_rows, HD), f32),
        pltpu.VMEM((img_rows, head_width), bf16),
        pltpu.VMEM((remotes, 2, heads, kv_rows, HD), bf16),
        pltpu.VMEM((heads, img_rows, 1), f32),
        pltpu.VMEM((heads, img_rows, 1), f32),
        pltpu.VMEM((heads, img_rows, HD), f32),
        pltpu.VMEM((heads, img_rows, HD), bf16),
        pltpu.VMEM((3, heads, img_rows, HD), bf16),
        pltpu.VMEM((3, head_width, cols), bf16),
        pltpu.VMEM((img_rows, cols), f32),
        pltpu.VMEM((img_rows, cols), bf16),
        pltpu.VMEM((img_rows, cols), bf16),
        pltpu.VMEM((img_rows, HD), f32),
        pltpu.VMEM((PLANE, out_rows, HD), f32),
        pltpu.VMEM((2, THIRDS, out_rows, HD), f32),
        pltpu.VMEM((8, HD), f32),
        pltpu.VMEM((2, THIRDS, 8, HD), f32),
        dma((15,)),
        dma((remotes, 2, heads)),
        dma((remotes, 2, heads)),
        dma((3,)),
        dma((3,)),
        dma((3,)),
        dma((3,)),
        dma((3, 2)),
        dma((3, 2)),
        dma((3, 4)),
        dma((3, 4)),
        dma((3, heads)),
        dma((3, heads)),
        dma((2, heads)),
        dma((PLANE,)),
        dma((2, THIRDS)),
        dma((PLANE,)),
        dma((2, THIRDS)),
    ]
    vmem = pl.BlockSpec(memory_space=pltpu.VMEM)
    smem = pl.BlockSpec(memory_space=pltpu.SMEM)
    anywhere = pl.BlockSpec(memory_space=pl.ANY)
    fresh, stepped = pl.pallas_call(
        functools.partial(kernel, n_patch),
        out_shape=(
            jax.ShapeDtypeStruct((2, kv_rows, head_width), bf16),
            jax.ShapeDtypeStruct((2, out_rows, channels), f32),
        ),
        in_specs=[anywhere] * len(args) + [smem] * 3,
        out_specs=(vmem, vmem),
        scratch_shapes=scratch,
        compiler_params=pltpu.CompilerParams(
            collective_id=0, has_side_effects=True, vmem_limit_bytes=VMEM_MAIN
        ),
    )(*args, guidance, step_index, step_count)
    fresh, next_latent, denoised = pl.pallas_call(
        deliver,
        out_shape=(
            jax.ShapeDtypeStruct(fresh.shape, bf16),
            jax.ShapeDtypeStruct(latent.shape, f32),
            jax.ShapeDtypeStruct(latent.shape, f32),
        ),
        in_specs=[anywhere, anywhere],
        out_specs=(anywhere, anywhere, anywhere),
        scratch_shapes=[
            pltpu.VMEM(fresh.shape, bf16),
            pltpu.VMEM(stepped.shape, f32),
            dma((2,)),
            dma((3,)),
        ],
        compiler_params=pltpu.CompilerParams(vmem_limit_bytes=VMEM_MAIN),
    )(fresh, stepped)
    return fresh[None], next_latent, denoised


def solution(mesh):
    return jax.shard_map(
        functools.partial(body, mesh.shape["patch"]),
        mesh=mesh,
        in_specs=(
            P("cfg", ("groups", "patch"), None),
            P("cfg", ("groups", "patch"), None),
            P(("groups", "cfg"), None, None),
            P(None, None, "head"),
            P(),
            P(),
            P("head", None),
            P(),
            P("cfg", None, ("groups", "patch"), "head"),
            P(("groups", "cfg"), None, None),
            P(),
            P(),
            P(("groups", "patch", "cfg", "head"), None),
            P(("groups", "patch", "cfg", "head"), None),
            P("groups"),
            P(),
            P(),
        ),
        out_specs=(
            P("cfg", None, ("groups", "patch"), "head"),
            P(("groups", "patch", "cfg", "head"), None),
            P(("groups", "patch", "cfg", "head"), None),
        ),
        check_vma=False,
    )
```

```python
import functools
import math

import jax
import jax.numpy as jnp
from jax import lax
from jax.experimental import pallas as pl
from jax.experimental.pallas import tpu as pltpu
from jax.sharding import PartitionSpec as P

HD = 128
GRID_W = 128
LN_ROWS = 16
LN_UNROLL = 4
THIRDS = 3
PLANE = 8
VMEM_MAIN = 67043328

epsilon = 1e-06
time_shift = 3.0
MESH = pl.DeviceIdType.MESH


def normed(values):
    centered = values - jnp.mean(values, axis=-1, keepdims=True)
    variance = jnp.mean(centered * centered, axis=-1, keepdims=True)
    return centered * lax.rsqrt(variance + epsilon)


def noise_level(index, count):
    frac = 1.0 - index / count
    lift = math.exp(time_shift)
    return lift * frac / (lift * frac + 1.0 - frac)


def log_ratio(sigma_val):
    return jnp.log(1.0 - sigma_val) - jnp.log(sigma_val)


def rotation_tables(cos_ref, sin_ref, txt_rows, first_pos):
    shape = cos_ref.shape
    quarter = HD // 4
    rows = lax.broadcasted_iota(jnp.int32, shape, 0)
    lanes = lax.broadcasted_iota(jnp.int32, shape, 1)
    pos = jnp.where(rows >= txt_rows, rows - txt_rows + first_pos, 0)
    place = jnp.where(lanes < 2 * quarter, pos // GRID_W, pos % GRID_W).astype(jnp.float32)
    step = (lanes % quarter).astype(jnp.float32)
    angle = place * jnp.exp(step * (-math.log(10000.0) / quarter))
    sine = jnp.sin(angle)
    cos_ref[...] = jnp.cos(angle)
    sin_ref[...] = jnp.where(lanes % (2 * quarter) < quarter, -sine, sine)


def rotated(values, gain, cosine, sine):
    quarter = HD // 4
    v = values * lax.rsqrt(jnp.mean(values * values, axis=-1, keepdims=True) + epsilon) * gain
    lanes = lax.broadcasted_iota(jnp.int32, v.shape, 1)
    swapped = jnp.where(
        lanes % (2 * quarter) < quarter,
        pltpu.roll(v, HD - quarter, 1),
        pltpu.roll(v, quarter, 1),
    )
    return (v * cosine + swapped * sine).astype(jnp.bfloat16)


def kernel(
    n_patch,
    hid, txt, mod, w_qkv, q_gain, k_gain, w_out, b_out, stale, fmod, w_fin, b_fin, lat, prev,
    guidance, step_index, step_count,
    fresh_s, step_o,
    stale_v, pair_v, hid_v, txt_v, mod_v, w_v, qg_v, kg_v, wo_v, bo_v, fmod_v, wf_v, bf_v, lat_v, prev_v,
    modded, proj, cos_s, sin_s, q_s, kv_s, m_s, l_s, acc_s, attn_s, attn_in,
    w_in, base_s, out_acc, hi_s, lo_s, stat_s, vel_s, vel_in, vec_s, vec_in,
    loc_sem, kv_send, kv_recv, wz_send, wz_recv, wx_send, wx_recv, wy_send, wy_recv,
    wc_send, wc_recv, at_send, at_recv, fw_send, v_send, v_recv, u_send, u_recv,
):
    patch = lax.axis_index("patch")
    group = lax.axis_index("groups")
    cfg = lax.axis_index("cfg")
    head = lax.axis_index("head")
    side = lax.div(head, 2)
    third = lax.rem(head, THIRDS)
    is_end = third == 0
    is_mid = third != 0
    mate = 2 * side + 1 - lax.rem(head, 2)
    partners = (mate, 3 - head, lax.rem(head + 2, 4))
    x_bit = lax.rem(patch, 2)
    x_dev = {"patch": patch + 1 - 2 * x_bit}
    y_dev = {"groups": 1 - group}
    c_dev = {"cfg": 1 - cfg}
    img_rows, d = hid_v.shape
    txt_rows = txt_v.shape[0]
    head_width = wo_v.shape[0]
    heads = head_width // HD
    out_rows = lat_v.shape[0]
    half = img_rows // 2
    cols = d // THIRDS
    share = head_width // PLANE
    my_cols = pl.ds(pl.multiple_of(third * cols, HD), cols)
    half_at = pl.ds(pl.multiple_of(side * half, half), half)

    pair_at = pl.ds(pl.multiple_of((cfg * 2 + group) * 2 * share, 16), 2 * share)
    first_pairs = [(stale, stale_v), (w_out.at[pair_at], pair_v)]
    pairs = [
        (mod, mod_v), (txt, txt_v), (hid, hid_v),
        (w_qkv.at[1], w_v.at[1]), (w_qkv.at[2], w_v.at[2]), (w_qkv.at[0], w_v.at[0]),
        (k_gain, kg_v), (q_gain, qg_v), (w_out.at[:, my_cols], wo_v), (b_out, bo_v),
        (fmod, fmod_v), (w_fin.at[:, my_cols], wf_v.at[pl.ds(0, w_fin.shape[0])]),
        (b_fin, bf_v), (lat, lat_v), (prev, prev_v),
    ]
    loads = [
        pltpu.make_async_copy(s, t, loc_sem.at[i]) for i, (s, t) in enumerate(first_pairs + pairs)
    ]
    for copy in loads:
        copy.start()
    local = loads[2:]

    def remote(source, target, send, recv, device):
        return pltpu.make_async_remote_copy(
            src_ref=source, dst_ref=target, send_sem=send, recv_sem=recv,
            device_id=device, device_id_type=MESH,
        )

    peers = [{"patch": lax.rem(patch + j, n_patch)} for j in range(1, n_patch)] + [y_dev]
    owners = [(dc, dh) for dc in range(2) for dh in range(4)]
    for dc, dh in owners[1:]:
        peers.append({"cfg": lax.rem(cfg + dc, 2), "head": lax.rem(head + dh, 4)})
    barrier = pltpu.get_barrier_semaphore()
    for peer in peers:
        pl.semaphore_signal(barrier, inc=1, device_id=peer, device_id_type=MESH)
    rotation_tables(cos_s, sin_s, txt_rows, patch * img_rows)
    loads[0].wait()
    loads[1].wait()
    pl.semaphore_wait(barrier, len(peers))

    def kv_copy(j, hh, which):
        return remote(
            stale_v.at[which, :, pl.ds(hh * HD, HD)], kv_s.at[j - 1, which, hh],
            kv_send.at[j - 1, which, hh], kv_recv.at[j - 1, which, hh],
            {"patch": lax.rem(patch + j, n_patch)},
        )

    for hh in range(heads):
        for which in range(2):
            for j in range(1, n_patch):
                kv_copy(j, hh, which).start()

    def unit(x, y, c):
        one = 1 - cfg if c else cfg
        two = 1 - group if y else group
        three = 1 - x_bit if x else x_bit
        return pl.ds(pl.multiple_of((one * 4 + two * 2 + three) * share, 16), share)

    own = unit(0, 0, 0)

    near = jnp.where(is_mid, 1, 2)
    slots = (0, near, 3 - near)

    def w_over_z(i, k=0):
        r, rows = slots[i], unit(k, 0, 0)
        to = mate if i == 0 else jnp.where(r == 1, partners[1], partners[2])
        at = pl.ds(pl.multiple_of(lax.rem(to, THIRDS) * cols, HD), cols)
        bit = 1 - x_bit if k else x_bit
        source = pl.ds(pl.multiple_of(bit * share, 16), share)
        return remote(
            pair_v.at[source, at], w_in.at[r, rows], wz_send.at[r, k], wz_recv.at[r, k], {"head": to}
        )

    def w_over_x(i, k):
        r = slots[i]
        at = w_in.at[r, unit(0, k, 0)]
        return remote(at, at, wx_send.at[r, k], wx_recv.at[r, k], x_dev)

    def w_over_y(i, k):
        r = slots[i]
        at = w_in.at[r, unit(k, 0, 0)]
        return remote(at, at, wy_send.at[r, k], wy_recv.at[r, k], y_dev)

    def w_over_c(i, k):
        r = slots[i]
        at = w_in.at[r, unit(k % 2, k // 2, 0)]
        return remote(at, at, wc_send.at[r, k], wc_recv.at[r, k], c_dev)

    z_units = ((0, 0), (1, 0), (2, 0), (0, 1))
    x_units = ((1, 0), (2, 0), (2, 1))
    y_units = ((0, 0), (1, 0), (2, 0), (0, 1), (1, 1))
    for i, k in z_units:
        w_over_z(i, k).start()

    def w_landed(i, k=0):
        w_over_z(i, k).wait_recv()
        if i:
            w_over_x(i, 0).start()
        w_over_y(i, k).start()
        w_over_c(i, k).start()

    def w_crossed(i, k=0):
        w_over_x(i, k).wait_recv()
        if i == 1:
            w_over_y(1, 1).start()
        w_over_c(i, 1 + 2 * k).start()

    def w_passed(i, k):
        w_over_y(i, k).wait_recv()
        if i == 2:
            w_over_x(2, 1).start()
        w_over_c(i, 2 + k).start()

    for copy in local[:3]:
        copy.wait()

    def modulate(values):
        out = normed(values.astype(jnp.float32)) * (1.0 + mod_v[1]) + mod_v[0]
        return out.astype(jnp.bfloat16)

    modded[pl.ds(0, txt_rows), :] = modulate(txt_v[...])

    def ln_step(i, carry):
        at = pl.multiple_of(i * LN_ROWS, LN_ROWS)
        modded[pl.ds(at + txt_rows, LN_ROWS), :] = modulate(hid_v[pl.ds(at, LN_ROWS), :])
        return carry

    lax.fori_loop(0, img_rows // LN_ROWS, ln_step, 0, unroll=LN_UNROLL)

    local[3].wait()
    local[6].wait()
    proj[...] = jnp.dot(modded[...], w_v[1], preferred_element_type=jnp.float32)
    for hh in range(heads):
        at = pl.ds(hh * HD, HD)
        fresh_s[0, :, at] = rotated(proj[:, at], kg_v[...], cos_s[...], sin_s[...])
    local[4].wait()
    fresh_s[1] = jnp.dot(modded[...], w_v[2], preferred_element_type=jnp.float32).astype(
        jnp.bfloat16
    )
    local[5].wait()
    local[7].wait()
    img_at = pl.ds(txt_rows, img_rows)
    proj[img_at, :] = jnp.dot(modded[img_at, :], w_v[0], preferred_element_type=jnp.float32)
    for hh in range(heads):
        at = pl.ds(hh * HD, HD)
        q_s[:, at] = rotated(proj[img_at, at], qg_v[...], cos_s[img_at, :], sin_s[img_at, :])

    w_landed(0)
    exp_scale = HD ** (-0.5) * math.log2(math.e)

    def scores_of(hh, keys):
        return (
            lax.dot_general(
                q_s[:, pl.ds(hh * HD, HD)],
                keys,
                (((1,), (1,)), ((), ())),
                preferred_element_type=jnp.float32,
            )
            * exp_scale
        )

    for hh in range(heads):
        at = pl.ds(hh * HD, HD)
        scores = scores_of(hh, fresh_s[0, :, at])
        top = jnp.max(scores, axis=-1, keepdims=True)
        expo = jnp.exp2(scores - top)
        m_s[hh] = top
        l_s[hh] = jnp.sum(expo, axis=-1, keepdims=True)
        acc_s[hh] = jnp.dot(
            expo.astype(jnp.bfloat16), fresh_s[1, :, at], preferred_element_type=jnp.float32
        )

    def f32(values):
        return values.astype(jnp.float32)

    for copy in local[8:]:
        copy.wait()
    channels = lat_v.shape[1]
    wf_v[pl.ds(channels, wf_v.shape[0] - channels), :] = jnp.zeros(
        (wf_v.shape[0] - channels, cols), jnp.bfloat16
    )
    scale_up = 1.0 + fmod_v[1:2, my_cols]
    shift_up = fmod_v[0:1, my_cols]
    lines = lax.broadcasted_iota(jnp.int32, (8, cols), 0)
    scale_hi, shift_hi = f32(scale_up.astype(jnp.bfloat16)), f32(shift_up.astype(jnp.bfloat16))
    rows_up = jnp.where(lines == 0, scale_hi, jnp.where(lines == 1, scale_up - scale_hi, 0.0))
    rows_up = jnp.where(lines == 2, shift_hi, jnp.where(lines == 3, shift_up - shift_hi, rows_up))

    def to_channels(values):
        return lax.dot_general(
            values, wf_v[...], (((1,), (1,)), ((), ())), preferred_element_type=jnp.float32
        )

    vec_s[...] = to_channels(rows_up.astype(jnp.bfloat16))

    def each_owner(act):
        for dc, dh in owners:
            to_cfg, to_head = lax.rem(cfg + dc, 2), lax.rem(head + dh, 4)
            wanted = is_mid | (to_cfg == side)
            slot = to_cfg * 4 + to_head
            where_to = {"cfg": to_cfg, "head": to_head}
            at = dc * 4 + dh

            @pl.when(wanted)
            def _():
                act(at, slot, where_to, dc == 0 and dh == 0)

    def vec_copy(at, where_to):
        return remote(
            vec_s, vec_in.at[cfg, third], u_send.at[at], u_recv.at[cfg, third], where_to
        )

    def vel_copy(at, slot, where_to):
        return remote(
            vel_s.at[slot], vel_in.at[cfg, third], v_send.at[at], v_recv.at[cfg, third], where_to
        )

    def vec_start(at, slot, where_to, mine):
        if mine:
            vec_in[cfg, third] = vec_s[...]
        else:
            vec_copy(at, where_to).start()

    each_owner(vec_start)

    def attn_full(r, hh):
        return remote(
            attn_s.at[hh], attn_in.at[r, hh], at_send.at[r, hh], at_recv.at[r, hh],
            {"head": partners[r]},
        )

    def attn_half(hh):
        return remote(
            attn_s.at[hh, half_at], attn_in.at[0, hh, half_at], at_send.at[0, hh],
            at_recv.at[0, hh], {"head": mate},
        )

    def attn_relay(r, hh):
        return remote(
            attn_in.at[r, hh, half_at], attn_in.at[3 - r, hh, half_at], fw_send.at[r - 1, hh],
            at_recv.at[3 - r, hh], {"head": mate},
        )

    def other_block(j, hh):
        scores = scores_of(hh, kv_s[j, 0, hh])
        old = m_s[hh]
        top = jnp.maximum(old, jnp.max(scores, axis=-1, keepdims=True))
        factor = jnp.exp2(old - top)
        expo = jnp.exp2(scores - top)
        m_s[hh] = top
        l_s[hh] = l_s[hh] * factor + jnp.sum(expo, axis=-1, keepdims=True)
        acc_s[hh] = acc_s[hh] * factor + jnp.dot(
            expo.astype(jnp.bfloat16), kv_s[j, 1, hh], preferred_element_type=jnp.float32
        )

    for hh in range(heads):
        for j in range(1, n_patch):
            for which in range(2):
                kv_copy(j, hh, which).wait_recv()
        if n_patch <= 2:
            for j in range(n_patch - 1):
                other_block(j, hh)
        else:
            lax.fori_loop(0, n_patch - 1, lambda j, c: (other_block(j, hh), c)[1], 0)
        attn_s[hh] = (acc_s[hh] / l_s[hh]).astype(jnp.bfloat16)

        @pl.when(is_end)
        def _():
            attn_full(2, hh).start()
            attn_full(0, hh).start()

        @pl.when(is_mid)
        def _():
            attn_full(1, hh).start()
            attn_half(hh).start()

        if hh == 0:
            w_landed(1)
        if hh == heads - 2:
            w_landed(2)

    w_landed(0, 1)

    def joined(ref, at):
        return jnp.concatenate([ref[hh, at, :] for hh in range(heads)], axis=1)

    def project(ref, weights, at):
        return jnp.dot(joined(ref, at), weights, preferred_element_type=jnp.float32)

    everything = pl.ds(0, img_rows)

    def on_rows(act):
        @pl.when(is_mid)
        def _():
            act(everything, img_rows)

        @pl.when(is_end)
        def _():
            act(half_at, half)

    def start_acc(at, count):
        out_acc[at, :] = project(attn_s, wo_v[...], at)

    gate = mod_v[2, :, my_cols]
    bias = bo_v[:, my_cols]

    def residual(at, count):
        base_s[at, :] = f32(hid_v[at, my_cols]) + gate * bias

    w_passed(0, 0)
    w_passed(1, 0)
    on_rows(start_acc)
    on_rows(residual)

    def pass_on(hh):
        @pl.when(is_mid)
        def _():
            for r in (1, 2):
                attn_full(r, hh).wait_recv()
                attn_relay(r, hh).start()

    def add_head(i):
        for k in range(4):
            w_over_c(i, k).wait_recv()
        r = slots[i]

        @pl.when(is_end)
        def _():
            for hh in range(heads):
                if i == 0:
                    attn_half(hh).wait_recv()
                else:
                    attn_relay(i, hh).wait_recv()

        @pl.when(is_mid)
        def _():
            if i == 0:
                for hh in range(heads):
                    attn_full(0, hh).wait_recv()

        def add_acc(at, count):
            out_acc[at, :] += project(attn_in.at[r], w_in[r], at)

        on_rows(add_acc)

    pass_on(0)
    w_crossed(1)
    w_passed(2, 0)
    for hh in range(1, heads - 1):
        pass_on(hh)
    w_crossed(2)
    w_passed(0, 1)
    w_crossed(2, 1)
    w_passed(1, 1)
    pass_on(heads - 1)
    add_head(0)
    add_head(1)
    add_head(2)

    lanes = lax.broadcasted_iota(jnp.int32, (LN_ROWS, HD), 1)

    def final_step(first):
        def run(i, carry):
            at = pl.ds(pl.multiple_of(first + i * LN_ROWS, LN_ROWS), LN_ROWS)
            mixed = base_s[at, :] + gate * out_acc[at, :]
            mean = jnp.mean(mixed, axis=-1, keepdims=True)
            centered = mixed - mean
            spread = jnp.sum(centered * centered, axis=-1, keepdims=True)
            scaled = centered * scale_up
            high = scaled.astype(jnp.bfloat16)
            hi_s[at, :] = high
            lo_s[at, :] = (scaled - f32(high)).astype(jnp.bfloat16)
            mean_hi, spread_hi = f32(mean.astype(jnp.bfloat16)), f32(spread.astype(jnp.bfloat16))
            stat = jnp.where(lanes == channels, mean_hi, 0.0)
            stat = jnp.where(lanes == channels + 1, mean - mean_hi, stat)
            stat = jnp.where(lanes == channels + 2, spread_hi, stat)
            stat_s[at, :] = jnp.where(lanes == channels + 3, spread - spread_hi, stat)
            return carry

        return run

    def finish(at, count):
        first = 0 if count == img_rows else side * half
        lax.fori_loop(0, count // LN_ROWS, final_step(first), 0, unroll=LN_UNROLL)
        value = to_channels(hi_s[at, :]) + to_channels(lo_s[at, :]) + stat_s[at, :]
        for i in range(count // out_rows):
            slot = i if count == img_rows else side * 4 + i
            vel_s[slot] = value[i * out_rows : (i + 1) * out_rows].astype(jnp.bfloat16)

    on_rows(finish)

    def vel_start(at, slot, where_to, mine):
        if mine:
            vel_in[cfg, third] = vel_s[slot]
        else:
            vel_copy(at, slot, where_to).start()

    each_owner(vel_start)

    ones = jnp.ones(lat_v.shape, jnp.float32)
    index = ones * step_index[0].astype(jnp.float32)
    count = ones * step_count[0].astype(jnp.float32)
    sigma_prev = noise_level(index - 1.0, count)
    sigma_now = noise_level(index, count)
    sigma_next = noise_level(index + 1.0, count)
    step_now = log_ratio(sigma_next) - log_ratio(sigma_now)
    step_prev = log_ratio(sigma_now) - log_ratio(sigma_prev)
    ratio = step_prev / step_now
    shrink = (1.0 - sigma_next) * (jnp.exp(-step_now) - 1.0)
    latent = lat_v[...]

    for b in range(2):
        for k in range(THIRDS):
            source = 3 * cfg if k == 0 else k

            @pl.when((cfg != b) | (head != source))
            def _():
                where_to = {"cfg": cfg, "head": head}
                for kind in (0, 1):
                    pltpu.make_async_remote_copy(
                        src_ref=vec_s if kind else vel_s.at[0],
                        dst_ref=vec_in.at[b, k] if kind else vel_in.at[b, k],
                        send_sem=u_send.at[0] if kind else v_send.at[0],
                        recv_sem=u_recv.at[b, k] if kind else v_recv.at[b, k],
                        device_id=c_dev,
                        device_id_type=MESH,
                    ).wait_recv()

    def velocity(b):
        parts = [f32(vel_in[b, k]) for k in range(THIRDS)]

        def stat_of(part, lane):
            return part[:, lane : lane + 1] + part[:, lane + 1 : lane + 2]

        means = [stat_of(part, channels) for part in parts]
        mean = sum(means) / THIRDS
        spread = sum(stat_of(part, channels + 2) for part in parts)
        spread = spread + cols * sum((m - mean) * (m - mean) for m in means)
        total = 0.0
        base = bf_v[...]
        for k in range(THIRDS):
            lift = vec_in[b, k, 0:1, :channels] + vec_in[b, k, 1:2, :channels]
            base = base + vec_in[b, k, 2:3, :channels] + vec_in[b, k, 3:4, :channels]
            total = total + parts[k][:, :channels] + (means[k] - mean) * lift
        return total * lax.rsqrt(spread / d + epsilon) + base

    cond, uncond = velocity(0), velocity(1)
    guided = uncond + guidance[0] * (cond - uncond)
    denoised = latent - sigma_now * guided
    blend = (1.0 + 0.5 / ratio) * denoised - 0.5 / ratio * prev_v[...]
    step_o[1] = denoised
    step_o[0] = sigma_next / sigma_now * latent - shrink * blend

    for hh in range(heads):
        for which in range(2):
            for j in range(1, n_patch):
                kv_copy(j, hh, which).wait_send()
    for i, k in z_units:
        w_over_z(i, k).wait_send()
    for i, k in x_units:
        w_over_x(i, k).wait_send()
    for i, k in y_units:
        w_over_y(i, k).wait_send()
    for i in range(3):
        for k in range(4):
            w_over_c(i, k).wait_send()

    @pl.when(is_end)
    def _():
        for hh in range(heads):
            attn_full(0, hh).wait_send()
            attn_full(2, hh).wait_send()

    @pl.when(is_mid)
    def _():
        for hh in range(heads):
            attn_full(1, hh).wait_send()
            attn_half(hh).wait_send()
            for s in (1, 2):
                attn_relay(s, hh).wait_send()

    def sent(at, slot, where_to, mine):
        if not mine:
            vec_copy(at, where_to).wait_send()
            vel_copy(at, slot, where_to).wait_send()

    each_owner(sent)


def deliver(fresh, stepped, fresh_o, next_o, den_o, fresh_v, step_v, in_sem, out_sem):
    loads = [
        pltpu.make_async_copy(stepped, step_v, in_sem.at[0]),
        pltpu.make_async_copy(fresh, fresh_v, in_sem.at[1]),
    ]
    for copy in loads:
        copy.start()
    pairs = ((step_v.at[0], next_o), (step_v.at[1], den_o), (fresh_v, fresh_o))
    stores = [pltpu.make_async_copy(s, t, out_sem.at[i]) for i, (s, t) in enumerate(pairs)]
    loads[0].wait()
    stores[0].start()
    stores[1].start()
    loads[1].wait()
    stores[2].start()
    for copy in stores:
        copy.wait()


def body(
    n_patch,
    img_hidden, txt_hidden, modulation, w_qkv, q_gain, k_gain, w_out, b_out, stale_kv,
    final_mod, w_final, b_final, latent, prev_denoised, guidance, step_index, step_count,
):
    bf16, f32 = jnp.bfloat16, jnp.float32
    img_rows, d = img_hidden.shape[1:]
    txt_rows = txt_hidden.shape[1]
    kv_rows = img_rows + txt_rows
    head_width = w_out.shape[0]
    heads = head_width // HD
    out_rows, channels = latent.shape
    cols = d // THIRDS
    args = (
        img_hidden[0],
        txt_hidden[0],
        modulation.transpose(1, 0, 2),
        w_qkv.transpose(1, 0, 2),
        q_gain[None],
        k_gain[None],
        w_out,
        b_out[None],
        stale_kv[0],
        final_mod[0],
        w_final.T,
        b_final[None],
        latent,
        prev_denoised,
    )
    dma = pltpu.SemaphoreType.DMA
    shapes = {6: (head_width, cols), 10: (HD, cols)}
    remotes = n_patch - 1
    scratch = [
        pltpu.VMEM((2, kv_rows, head_width), bf16),
        pltpu.VMEM((2 * head_width // PLANE, d), bf16),
    ] + [
        pltpu.VMEM(shapes.get(i, a.shape), a.dtype) for i, a in enumerate(args) if i != 8
    ] + [
        pltpu.VMEM((kv_rows, d), bf16),
        pltpu.VMEM((kv_rows, head_width), f32),
        pltpu.VMEM((kv_rows, HD), f32),
        pltpu.VMEM((kv_rows, HD), f32),
        pltpu.VMEM((img_rows, head_width), bf16),
        pltpu.VMEM((remotes, 2, heads, kv_rows, HD), bf16),
        pltpu.VMEM((heads, img_rows, 1), f32),
        pltpu.VMEM((heads, img_rows, 1), f32),
        pltpu.VMEM((heads, img_rows, HD), f32),
        pltpu.VMEM((heads, img_rows, HD), bf16),
        pltpu.VMEM((3, heads, img_rows, HD), bf16),
        pltpu.VMEM((3, head_width, cols), bf16),
        pltpu.VMEM((img_rows, cols), f32),
        pltpu.VMEM((img_rows, cols), f32),
        pltpu.VMEM((img_rows, cols), bf16),
        pltpu.VMEM((img_rows, cols), bf16),
        pltpu.VMEM((img_rows, HD), f32),
        pltpu.VMEM((PLANE, out_rows, HD), bf16),
        pltpu.VMEM((2, THIRDS, out_rows, HD), bf16),
        pltpu.VMEM((8, HD), f32),
        pltpu.VMEM((2, THIRDS, 8, HD), f32),
        dma((17,)),
        dma((remotes, 2, heads)),
        dma((remotes, 2, heads)),
        dma((3, 2)),
        dma((3, 2)),
        dma((3, 2)),
        dma((3, 2)),
        dma((3, 2)),
        dma((3, 2)),
        dma((3, 4)),
        dma((3, 4)),
        dma((3, heads)),
        dma((3, heads)),
        dma((2, heads)),
        dma((PLANE,)),
        dma((2, THIRDS)),
        dma((PLANE,)),
        dma((2, THIRDS)),
    ]
    vmem = pl.BlockSpec(memory_space=pltpu.VMEM)
    smem = pl.BlockSpec(memory_space=pltpu.SMEM)
    anywhere = pl.BlockSpec(memory_space=pl.ANY)
    fresh, stepped = pl.pallas_call(
        functools.partial(kernel, n_patch),
        out_shape=(
            jax.ShapeDtypeStruct((2, kv_rows, head_width), bf16),
            jax.ShapeDtypeStruct((2, out_rows, channels), f32),
        ),
        in_specs=[anywhere] * len(args) + [smem] * 3,
        out_specs=(vmem, vmem),
        scratch_shapes=scratch,
        compiler_params=pltpu.CompilerParams(
            collective_id=0, has_side_effects=True, vmem_limit_bytes=VMEM_MAIN
        ),
    )(*args, guidance, step_index, step_count)
    fresh, next_latent, denoised = pl.pallas_call(
        deliver,
        out_shape=(
            jax.ShapeDtypeStruct(fresh.shape, bf16),
            jax.ShapeDtypeStruct(latent.shape, f32),
            jax.ShapeDtypeStruct(latent.shape, f32),
        ),
        in_specs=[anywhere, anywhere],
        out_specs=(anywhere, anywhere, anywhere),
        scratch_shapes=[
            pltpu.VMEM(fresh.shape, bf16),
            pltpu.VMEM(stepped.shape, f32),
            dma((2,)),
            dma((3,)),
        ],
        compiler_params=pltpu.CompilerParams(vmem_limit_bytes=VMEM_MAIN),
    )(fresh, stepped)
    return fresh[None], next_latent, denoised


def solution(mesh):
    return jax.shard_map(
        functools.partial(body, mesh.shape["patch"]),
        mesh=mesh,
        in_specs=(
            P("cfg", ("groups", "patch"), None),
            P("cfg", ("groups", "patch"), None),
            P(("groups", "cfg"), None, None),
            P(None, None, "head"),
            P(),
            P(),
            P("head", None),
            P(),
            P("cfg", None, ("groups", "patch"), "head"),
            P(("groups", "cfg"), None, None),
            P(),
            P(),
            P(("groups", "patch", "cfg", "head"), None),
            P(("groups", "patch", "cfg", "head"), None),
            P("groups"),
            P(),
            P(),
        ),
        out_specs=(
            P("cfg", None, ("groups", "patch"), "head"),
            P(("groups", "patch", "cfg", "head"), None),
            P(("groups", "patch", "cfg", "head"), None),
        ),
        check_vma=False,
    )
```

```python
import functools
import math

import jax
import jax.numpy as jnp
from jax import lax
from jax.experimental import pallas as pl
from jax.experimental.pallas import tpu as pltpu
from jax.sharding import PartitionSpec as P

HD = 128
GRID_W = 128
LN_ROWS = 16
LN_UNROLL = 4
THIRDS = 3
PLANE = 8
VMEM_MAIN = 41943040
VMEM_DELIVER = 8388608

epsilon = 1e-06
time_shift = 3.0
MESH = pl.DeviceIdType.MESH


def normed(values):
    centered = values - jnp.mean(values, axis=-1, keepdims=True)
    variance = jnp.mean(centered * centered, axis=-1, keepdims=True)
    return centered * lax.rsqrt(variance + epsilon)


def noise_level(index, count):
    frac = 1.0 - index / count
    lift = math.exp(time_shift)
    return lift * frac / (lift * frac + 1.0 - frac)


def log_ratio(sigma_val):
    return jnp.log(1.0 - sigma_val) - jnp.log(sigma_val)


def rotation_tables(cos_ref, sin_ref, txt_rows, first_pos):
    shape = cos_ref.shape
    quarter = HD // 4
    rows = lax.broadcasted_iota(jnp.int32, shape, 0)
    lanes = lax.broadcasted_iota(jnp.int32, shape, 1)
    pos = jnp.where(rows >= txt_rows, rows - txt_rows + first_pos, 0)
    place = jnp.where(lanes < 2 * quarter, pos // GRID_W, pos % GRID_W).astype(jnp.float32)
    step = (lanes % quarter).astype(jnp.float32)
    angle = place * jnp.exp(step * (-math.log(10000.0) / quarter))
    sine = jnp.sin(angle)
    cos_ref[...] = jnp.cos(angle)
    sin_ref[...] = jnp.where(lanes % (2 * quarter) < quarter, -sine, sine)


def rotated(values, gain, cosine, sine):
    quarter = HD // 4
    v = values * lax.rsqrt(jnp.mean(values * values, axis=-1, keepdims=True) + epsilon) * gain
    lanes = lax.broadcasted_iota(jnp.int32, v.shape, 1)
    swapped = jnp.where(
        lanes % (2 * quarter) < quarter,
        pltpu.roll(v, HD - quarter, 1),
        pltpu.roll(v, quarter, 1),
    )
    return (v * cosine + swapped * sine).astype(jnp.bfloat16)


def kernel(
    n_patch,
    hid, txt, mod, w_qkv, q_gain, k_gain, w_out, b_out, stale, fmod, w_fin, b_fin, lat, prev,
    guidance, step_index, step_count,
    fresh_s, step_o,
    stale_v, pair_v, hid_v, txt_v, mod_v, w_v, qg_v, kg_v, wo_v, bo_v, fmod_v, wf_v, bf_v, lat_v, prev_v,
    modded, proj, cos_s, sin_s, q_s, kv_s, m_s, l_s, acc_s, attn_s, attn_in,
    w_in, base_s, out_acc, hi_s, lo_s, stat_s, vel_s, vel_in, vec_s, vec_in,
    loc_sem, kv_send, kv_recv, wz_send, wz_recv, wx_send, wx_recv, wy_send, wy_recv,
    wc_send, wc_recv, at_send, at_recv, fw_send, v_send, v_recv, u_send, u_recv,
):
    patch = lax.axis_index("patch")
    group = lax.axis_index("groups")
    cfg = lax.axis_index("cfg")
    head = lax.axis_index("head")
    side = lax.div(head, 2)
    third = lax.rem(head, THIRDS)
    is_end = third == 0
    is_mid = third != 0
    mate = 2 * side + 1 - lax.rem(head, 2)
    partners = (mate, 3 - head, lax.rem(head + 2, 4))
    x_bit = lax.rem(patch, 2)
    x_dev = {"patch": patch + 1 - 2 * x_bit}
    y_dev = {"groups": 1 - group}
    c_dev = {"cfg": 1 - cfg}
    img_rows, d = hid_v.shape
    txt_rows = txt_v.shape[0]
    head_width = wo_v.shape[0]
    heads = head_width // HD
    out_rows = lat_v.shape[0]
    half = img_rows // 2
    cols = d // THIRDS
    share = head_width // PLANE
    my_cols = pl.ds(pl.multiple_of(third * cols, HD), cols)
    half_at = pl.ds(pl.multiple_of(side * half, half), half)

    pair_at = pl.ds(pl.multiple_of((cfg * 2 + group) * 2 * share, 16), 2 * share)
    first_pairs = [(stale, stale_v), (w_out.at[pair_at], pair_v)]
    pairs = [
        (mod, mod_v), (txt, txt_v), (hid, hid_v),
        (w_qkv.at[1], w_v.at[1]), (w_qkv.at[2], w_v.at[2]), (w_qkv.at[0], w_v.at[0]),
        (k_gain, kg_v), (q_gain, qg_v), (w_out.at[:, my_cols], wo_v), (b_out, bo_v),
        (fmod, fmod_v), (w_fin.at[:, my_cols], wf_v.at[pl.ds(0, w_fin.shape[0])]),
        (b_fin, bf_v), (lat, lat_v), (prev, prev_v),
    ]
    loads = [
        pltpu.make_async_copy(s, t, loc_sem.at[i]) for i, (s, t) in enumerate(first_pairs + pairs)
    ]
    for copy in loads:
        copy.start()
    local = loads[2:]

    def remote(source, target, send, recv, device):
        return pltpu.make_async_remote_copy(
            src_ref=source, dst_ref=target, send_sem=send, recv_sem=recv,
            device_id=device, device_id_type=MESH,
        )

    peers = [{"patch": lax.rem(patch + j, n_patch)} for j in range(1, n_patch)] + [y_dev]
    owners = [(dc, dh) for dc in range(2) for dh in range(4)]
    for dc, dh in owners[1:]:
        peers.append({"cfg": lax.rem(cfg + dc, 2), "head": lax.rem(head + dh, 4)})
    barrier = pltpu.get_barrier_semaphore()
    for peer in peers:
        pl.semaphore_signal(barrier, inc=1, device_id=peer, device_id_type=MESH)
    rotation_tables(cos_s, sin_s, txt_rows, patch * img_rows)
    loads[0].wait()
    loads[1].wait()
    pl.semaphore_wait(barrier, len(peers))

    def kv_copy(j, hh, which):
        return remote(
            stale_v.at[which, :, pl.ds(hh * HD, HD)], kv_s.at[j - 1, which, hh],
            kv_send.at[j - 1, which, hh], kv_recv.at[j - 1, which, hh],
            {"patch": lax.rem(patch + j, n_patch)},
        )

    for hh in range(heads):
        for which in range(2):
            for j in range(1, n_patch):
                kv_copy(j, hh, which).start()

    def unit(x, y, c):
        one = 1 - cfg if c else cfg
        two = 1 - group if y else group
        three = 1 - x_bit if x else x_bit
        return pl.ds(pl.multiple_of((one * 4 + two * 2 + three) * share, 16), share)

    own = unit(0, 0, 0)

    near = jnp.where(is_mid, 1, 2)
    slots = (0, near, 3 - near)

    def w_over_z(i, k=0):
        r, rows = slots[i], unit(k, 0, 0)
        to = mate if i == 0 else jnp.where(r == 1, partners[1], partners[2])
        at = pl.ds(pl.multiple_of(lax.rem(to, THIRDS) * cols, HD), cols)
        bit = 1 - x_bit if k else x_bit
        source = pl.ds(pl.multiple_of(bit * share, 16), share)
        return remote(
            pair_v.at[source, at], w_in.at[r, rows], wz_send.at[r, k], wz_recv.at[r, k], {"head": to}
        )

    def w_over_x(i, k):
        r = slots[i]
        at = w_in.at[r, unit(0, k, 0)]
        return remote(at, at, wx_send.at[r, k], wx_recv.at[r, k], x_dev)

    def w_over_y(i, k):
        r = slots[i]
        at = w_in.at[r, unit(k, 0, 0)]
        return remote(at, at, wy_send.at[r, k], wy_recv.at[r, k], y_dev)

    def w_over_c(i, k):
        r = slots[i]
        at = w_in.at[r, unit(k % 2, k // 2, 0)]
        return remote(at, at, wc_send.at[r, k], wc_recv.at[r, k], c_dev)

    z_units = ((0, 0), (1, 0), (2, 0), (0, 1))
    x_units = ((1, 0), (2, 0), (2, 1))
    y_units = ((0, 0), (1, 0), (2, 0), (0, 1), (1, 1))
    for i, k in z_units:
        w_over_z(i, k).start()

    def w_landed(i, k=0):
        w_over_z(i, k).wait_recv()
        if i:
            w_over_x(i, 0).start()
        w_over_y(i, k).start()
        w_over_c(i, k).start()

    def w_crossed(i, k=0):
        w_over_x(i, k).wait_recv()
        if i == 1:
            w_over_y(1, 1).start()
        w_over_c(i, 1 + 2 * k).start()

    def w_passed(i, k):
        w_over_y(i, k).wait_recv()
        if i == 2:
            w_over_x(2, 1).start()
        w_over_c(i, 2 + k).start()

    for copy in local[:3]:
        copy.wait()

    def modulate(values):
        out = normed(values.astype(jnp.float32)) * (1.0 + mod_v[1]) + mod_v[0]
        return out.astype(jnp.bfloat16)

    modded[pl.ds(0, txt_rows), :] = modulate(txt_v[...])

    def ln_step(i, carry):
        at = pl.multiple_of(i * LN_ROWS, LN_ROWS)
        modded[pl.ds(at + txt_rows, LN_ROWS), :] = modulate(hid_v[pl.ds(at, LN_ROWS), :])
        return carry

    lax.fori_loop(0, img_rows // LN_ROWS, ln_step, 0, unroll=LN_UNROLL)

    local[3].wait()
    local[6].wait()
    proj[...] = jnp.dot(modded[...], w_v[1], preferred_element_type=jnp.float32)
    for hh in range(heads):
        at = pl.ds(hh * HD, HD)
        fresh_s[0, :, at] = rotated(proj[:, at], kg_v[...], cos_s[...], sin_s[...])
    local[4].wait()
    fresh_s[1] = jnp.dot(modded[...], w_v[2], preferred_element_type=jnp.float32).astype(
        jnp.bfloat16
    )
    local[5].wait()
    local[7].wait()
    img_at = pl.ds(txt_rows, img_rows)
    proj[img_at, :] = jnp.dot(modded[img_at, :], w_v[0], preferred_element_type=jnp.float32)
    for hh in range(heads):
        at = pl.ds(hh * HD, HD)
        q_s[:, at] = rotated(proj[img_at, at], qg_v[...], cos_s[img_at, :], sin_s[img_at, :])

    w_landed(0)
    exp_scale = HD ** (-0.5) * math.log2(math.e)

    def scores_of(hh, keys):
        return (
            lax.dot_general(
                q_s[:, pl.ds(hh * HD, HD)],
                keys,
                (((1,), (1,)), ((), ())),
                preferred_element_type=jnp.float32,
            )
            * exp_scale
        )

    for hh in range(heads):
        at = pl.ds(hh * HD, HD)
        scores = scores_of(hh, fresh_s[0, :, at])
        top = jnp.max(scores, axis=-1, keepdims=True)
        expo = jnp.exp2(scores - top)
        m_s[hh] = top
        l_s[hh] = jnp.sum(expo, axis=-1, keepdims=True)
        acc_s[hh] = jnp.dot(
            expo.astype(jnp.bfloat16), fresh_s[1, :, at], preferred_element_type=jnp.float32
        )

    def f32(values):
        return values.astype(jnp.float32)

    for copy in local[8:]:
        copy.wait()
    channels = lat_v.shape[1]
    wf_v[pl.ds(channels, wf_v.shape[0] - channels), :] = jnp.zeros(
        (wf_v.shape[0] - channels, cols), jnp.bfloat16
    )
    scale_up = 1.0 + fmod_v[1:2, my_cols]
    shift_up = fmod_v[0:1, my_cols]
    lines = lax.broadcasted_iota(jnp.int32, (8, cols), 0)
    scale_hi, shift_hi = f32(scale_up.astype(jnp.bfloat16)), f32(shift_up.astype(jnp.bfloat16))
    rows_up = jnp.where(lines == 0, scale_hi, jnp.where(lines == 1, scale_up - scale_hi, 0.0))
    rows_up = jnp.where(lines == 2, shift_hi, jnp.where(lines == 3, shift_up - shift_hi, rows_up))

    def to_channels(values):
        return lax.dot_general(
            values, wf_v[...], (((1,), (1,)), ((), ())), preferred_element_type=jnp.float32
        )

    vec_s[...] = to_channels(rows_up.astype(jnp.bfloat16))

    def each_owner(act):
        for dc, dh in owners:
            to_cfg, to_head = lax.rem(cfg + dc, 2), lax.rem(head + dh, 4)
            wanted = is_mid | (to_cfg == side)
            slot = to_cfg * 4 + to_head
            where_to = {"cfg": to_cfg, "head": to_head}
            at = dc * 4 + dh

            @pl.when(wanted)
            def _():
                act(at, slot, where_to, dc == 0 and dh == 0)

    def vec_copy(at, where_to):
        return remote(
            vec_s, vec_in.at[cfg, third], u_send.at[at], u_recv.at[cfg, third], where_to
        )

    def vel_copy(at, slot, where_to):
        return remote(
            vel_s.at[slot], vel_in.at[cfg, third], v_send.at[at], v_recv.at[cfg, third], where_to
        )

    def vec_start(at, slot, where_to, mine):
        if mine:
            vec_in[cfg, third] = vec_s[...]
        else:
            vec_copy(at, where_to).start()

    each_owner(vec_start)

    def attn_full(r, hh):
        return remote(
            attn_s.at[hh], attn_in.at[r, hh], at_send.at[r, hh], at_recv.at[r, hh],
            {"head": partners[r]},
        )

    def attn_half(hh):
        return remote(
            attn_s.at[hh, half_at], attn_in.at[0, hh, half_at], at_send.at[0, hh],
            at_recv.at[0, hh], {"head": mate},
        )

    def attn_relay(r, hh):
        return remote(
            attn_in.at[r, hh, half_at], attn_in.at[3 - r, hh, half_at], fw_send.at[r - 1, hh],
            at_recv.at[3 - r, hh], {"head": mate},
        )

    def other_block(j, hh):
        scores = scores_of(hh, kv_s[j, 0, hh])
        old = m_s[hh]
        top = jnp.maximum(old, jnp.max(scores, axis=-1, keepdims=True))
        factor = jnp.exp2(old - top)
        expo = jnp.exp2(scores - top)
        m_s[hh] = top
        l_s[hh] = l_s[hh] * factor + jnp.sum(expo, axis=-1, keepdims=True)
        acc_s[hh] = acc_s[hh] * factor + jnp.dot(
            expo.astype(jnp.bfloat16), kv_s[j, 1, hh], preferred_element_type=jnp.float32
        )

    for hh in range(heads):
        for j in range(1, n_patch):
            for which in range(2):
                kv_copy(j, hh, which).wait_recv()
        if n_patch <= 2:
            for j in range(n_patch - 1):
                other_block(j, hh)
        else:
            lax.fori_loop(0, n_patch - 1, lambda j, c: (other_block(j, hh), c)[1], 0)
        attn_s[hh] = (acc_s[hh] / l_s[hh]).astype(jnp.bfloat16)

        @pl.when(is_end)
        def _():
            attn_full(2, hh).start()
            attn_full(0, hh).start()

        @pl.when(is_mid)
        def _():
            attn_full(1, hh).start()
            attn_half(hh).start()

        if hh == 0:
            w_landed(1)
        if hh == heads - 2:
            w_landed(2)

    w_landed(0, 1)

    def joined(ref, at):
        return jnp.concatenate([ref[hh, at, :] for hh in range(heads)], axis=1)

    def project(ref, weights, at):
        return jnp.dot(joined(ref, at), weights, preferred_element_type=jnp.float32)

    everything = pl.ds(0, img_rows)

    def on_rows(act):
        @pl.when(is_mid)
        def _():
            act(everything, img_rows)

        @pl.when(is_end)
        def _():
            act(half_at, half)

    def start_acc(at, count):
        out_acc[at, :] = project(attn_s, wo_v[...], at)

    gate = mod_v[2, :, my_cols]
    bias = bo_v[:, my_cols]

    def residual(at, count):
        base_s[at, :] = f32(hid_v[at, my_cols]) + gate * bias

    w_passed(0, 0)
    w_passed(1, 0)
    on_rows(start_acc)
    on_rows(residual)

    def pass_on(hh):
        @pl.when(is_mid)
        def _():
            for r in (1, 2):
                attn_full(r, hh).wait_recv()
                attn_relay(r, hh).start()

    def add_head(i):
        for k in range(4):
            w_over_c(i, k).wait_recv()
        r = slots[i]

        @pl.when(is_end)
        def _():
            for hh in range(heads):
                if i == 0:
                    attn_half(hh).wait_recv()
                else:
                    attn_relay(i, hh).wait_recv()

        @pl.when(is_mid)
        def _():
            if i == 0:
                for hh in range(heads):
                    attn_full(0, hh).wait_recv()

        def add_acc(at, count):
            out_acc[at, :] += project(attn_in.at[r], w_in[r], at)

        on_rows(add_acc)

    pass_on(0)
    w_crossed(1)
    w_passed(2, 0)
    for hh in range(1, heads - 1):
        pass_on(hh)
    w_crossed(2)
    w_passed(0, 1)
    w_crossed(2, 1)
    w_passed(1, 1)
    pass_on(heads - 1)
    add_head(0)
    add_head(1)
    add_head(2)

    lanes = lax.broadcasted_iota(jnp.int32, (LN_ROWS, HD), 1)

    def final_step(first):
        def run(i, carry):
            at = pl.ds(pl.multiple_of(first + i * LN_ROWS, LN_ROWS), LN_ROWS)
            mixed = base_s[at, :] + gate * out_acc[at, :]
            mean = jnp.mean(mixed, axis=-1, keepdims=True)
            centered = mixed - mean
            spread = jnp.sum(centered * centered, axis=-1, keepdims=True)
            scaled = centered * scale_up
            high = scaled.astype(jnp.bfloat16)
            hi_s[at, :] = high
            lo_s[at, :] = (scaled - f32(high)).astype(jnp.bfloat16)
            mean_hi, spread_hi = f32(mean.astype(jnp.bfloat16)), f32(spread.astype(jnp.bfloat16))
            stat = jnp.where(lanes == channels, mean_hi, 0.0)
            stat = jnp.where(lanes == channels + 1, mean - mean_hi, stat)
            stat = jnp.where(lanes == channels + 2, spread_hi, stat)
            stat_s[at, :] = jnp.where(lanes == channels + 3, spread - spread_hi, stat)
            return carry

        return run

    def finish(at, count):
        first = 0 if count == img_rows else side * half
        lax.fori_loop(0, count // LN_ROWS, final_step(first), 0, unroll=LN_UNROLL)
        value = to_channels(hi_s[at, :]) + to_channels(lo_s[at, :]) + stat_s[at, :]
        for i in range(count // out_rows):
            slot = i if count == img_rows else side * 4 + i
            vel_s[slot] = value[i * out_rows : (i + 1) * out_rows].astype(jnp.bfloat16)

    on_rows(finish)

    def vel_start(at, slot, where_to, mine):
        if mine:
            vel_in[cfg, third] = vel_s[slot]
        else:
            vel_copy(at, slot, where_to).start()

    each_owner(vel_start)

    ones = jnp.ones(lat_v.shape, jnp.float32)
    index = ones * step_index[0].astype(jnp.float32)
    count = ones * step_count[0].astype(jnp.float32)
    sigma_prev = noise_level(index - 1.0, count)
    sigma_now = noise_level(index, count)
    sigma_next = noise_level(index + 1.0, count)
    step_now = log_ratio(sigma_next) - log_ratio(sigma_now)
    step_prev = log_ratio(sigma_now) - log_ratio(sigma_prev)
    ratio = step_prev / step_now
    shrink = (1.0 - sigma_next) * (jnp.exp(-step_now) - 1.0)
    latent = lat_v[...]

    for b in range(2):
        for k in range(THIRDS):
            source = 3 * cfg if k == 0 else k

            @pl.when((cfg != b) | (head != source))
            def _():
                where_to = {"cfg": cfg, "head": head}
                for kind in (0, 1):
                    pltpu.make_async_remote_copy(
                        src_ref=vec_s if kind else vel_s.at[0],
                        dst_ref=vec_in.at[b, k] if kind else vel_in.at[b, k],
                        send_sem=u_send.at[0] if kind else v_send.at[0],
                        recv_sem=u_recv.at[b, k] if kind else v_recv.at[b, k],
                        device_id=c_dev,
                        device_id_type=MESH,
                    ).wait_recv()

    def velocity(b):
        parts = [f32(vel_in[b, k]) for k in range(THIRDS)]

        def stat_of(part, lane):
            return part[:, lane : lane + 1] + part[:, lane + 1 : lane + 2]

        means = [stat_of(part, channels) for part in parts]
        mean = sum(means) / THIRDS
        spread = sum(stat_of(part, channels + 2) for part in parts)
        spread = spread + cols * sum((m - mean) * (m - mean) for m in means)
        total = 0.0
        base = bf_v[...]
        for k in range(THIRDS):
            lift = vec_in[b, k, 0:1, :channels] + vec_in[b, k, 1:2, :channels]
            base = base + vec_in[b, k, 2:3, :channels] + vec_in[b, k, 3:4, :channels]
            total = total + parts[k][:, :channels] + (means[k] - mean) * lift
        return total * lax.rsqrt(spread / d + epsilon) + base

    cond, uncond = velocity(0), velocity(1)
    guided = uncond + guidance[0] * (cond - uncond)
    denoised = latent - sigma_now * guided
    blend = (1.0 + 0.5 / ratio) * denoised - 0.5 / ratio * prev_v[...]
    step_o[1] = denoised
    step_o[0] = sigma_next / sigma_now * latent - shrink * blend

    for hh in range(heads):
        for which in range(2):
            for j in range(1, n_patch):
                kv_copy(j, hh, which).wait_send()
    for i, k in z_units:
        w_over_z(i, k).wait_send()
    for i, k in x_units:
        w_over_x(i, k).wait_send()
    for i, k in y_units:
        w_over_y(i, k).wait_send()
    for i in range(3):
        for k in range(4):
            w_over_c(i, k).wait_send()

    @pl.when(is_end)
    def _():
        for hh in range(heads):
            attn_full(0, hh).wait_send()
            attn_full(2, hh).wait_send()

    @pl.when(is_mid)
    def _():
        for hh in range(heads):
            attn_full(1, hh).wait_send()
            attn_half(hh).wait_send()
            for s in (1, 2):
                attn_relay(s, hh).wait_send()

    def sent(at, slot, where_to, mine):
        if not mine:
            vec_copy(at, where_to).wait_send()
            vel_copy(at, slot, where_to).wait_send()

    each_owner(sent)


def deliver(fresh, stepped, fresh_o, next_o, den_o, out_sem):
    pairs = ((fresh, fresh_o), (stepped.at[0], next_o), (stepped.at[1], den_o))
    stores = [pltpu.make_async_copy(s, t, out_sem.at[i]) for i, (s, t) in enumerate(pairs)]
    for copy in stores:
        copy.start()
    for copy in stores:
        copy.wait()


def body(
    n_patch,
    img_hidden, txt_hidden, modulation, w_qkv, q_gain, k_gain, w_out, b_out, stale_kv,
    final_mod, w_final, b_final, latent, prev_denoised, guidance, step_index, step_count,
):
    bf16, f32 = jnp.bfloat16, jnp.float32
    img_rows, d = img_hidden.shape[1:]
    txt_rows = txt_hidden.shape[1]
    kv_rows = img_rows + txt_rows
    head_width = w_out.shape[0]
    heads = head_width // HD
    out_rows, channels = latent.shape
    cols = d // THIRDS
    args = (
        img_hidden[0],
        txt_hidden[0],
        modulation.transpose(1, 0, 2),
        w_qkv.transpose(1, 0, 2),
        q_gain[None],
        k_gain[None],
        w_out,
        b_out[None],
        stale_kv[0],
        final_mod[0],
        w_final.T,
        b_final[None],
        latent,
        prev_denoised,
    )
    dma = pltpu.SemaphoreType.DMA
    shapes = {6: (head_width, cols), 10: (HD, cols)}
    remotes = n_patch - 1
    scratch = [
        pltpu.VMEM((2, kv_rows, head_width), bf16),
        pltpu.VMEM((2 * head_width // PLANE, d), bf16),
    ] + [
        pltpu.VMEM(shapes.get(i, a.shape), a.dtype) for i, a in enumerate(args) if i != 8
    ] + [
        pltpu.VMEM((kv_rows, d), bf16),
        pltpu.VMEM((kv_rows, head_width), f32),
        pltpu.VMEM((kv_rows, HD), f32),
        pltpu.VMEM((kv_rows, HD), f32),
        pltpu.VMEM((img_rows, head_width), bf16),
        pltpu.VMEM((remotes, 2, heads, kv_rows, HD), bf16),
        pltpu.VMEM((heads, img_rows, 1), f32),
        pltpu.VMEM((heads, img_rows, 1), f32),
        pltpu.VMEM((heads, img_rows, HD), f32),
        pltpu.VMEM((heads, img_rows, HD), bf16),
        pltpu.VMEM((3, heads, img_rows, HD), bf16),
        pltpu.VMEM((3, head_width, cols), bf16),
        pltpu.VMEM((img_rows, cols), f32),
        pltpu.VMEM((img_rows, cols), f32),
        pltpu.VMEM((img_rows, cols), bf16),
        pltpu.VMEM((img_rows, cols), bf16),
        pltpu.VMEM((img_rows, HD), f32),
        pltpu.VMEM((PLANE, out_rows, HD), bf16),
        pltpu.VMEM((2, THIRDS, out_rows, HD), bf16),
        pltpu.VMEM((8, HD), f32),
        pltpu.VMEM((2, THIRDS, 8, HD), f32),
        dma((17,)),
        dma((remotes, 2, heads)),
        dma((remotes, 2, heads)),
        dma((3, 2)),
        dma((3, 2)),
        dma((3, 2)),
        dma((3, 2)),
        dma((3, 2)),
        dma((3, 2)),
        dma((3, 4)),
        dma((3, 4)),
        dma((3, heads)),
        dma((3, heads)),
        dma((2, heads)),
        dma((PLANE,)),
        dma((2, THIRDS)),
        dma((PLANE,)),
        dma((2, THIRDS)),
    ]
    vmem = pl.BlockSpec(memory_space=pltpu.VMEM)
    smem = pl.BlockSpec(memory_space=pltpu.SMEM)
    anywhere = pl.BlockSpec(memory_space=pl.ANY)
    operands = [pltpu.with_memory_space_constraint(a, pltpu.HBM) for a in args]
    fresh, stepped = pl.pallas_call(
        functools.partial(kernel, n_patch),
        out_shape=(
            pltpu.VMEM((2, kv_rows, head_width), bf16),
            pltpu.VMEM((2, out_rows, channels), f32),
        ),
        in_specs=[anywhere] * len(args) + [smem] * 3,
        out_specs=(vmem, vmem),
        scratch_shapes=scratch,
        compiler_params=pltpu.CompilerParams(
            collective_id=0, has_side_effects=True, vmem_limit_bytes=VMEM_MAIN
        ),
    )(*operands, guidance, step_index, step_count)
    fresh, next_latent, denoised = pl.pallas_call(
        deliver,
        out_shape=(
            jax.ShapeDtypeStruct(fresh.shape, bf16),
            jax.ShapeDtypeStruct(latent.shape, f32),
            jax.ShapeDtypeStruct(latent.shape, f32),
        ),
        in_specs=[vmem, vmem],
        out_specs=(anywhere, anywhere, anywhere),
        scratch_shapes=[dma((3,))],
        compiler_params=pltpu.CompilerParams(vmem_limit_bytes=VMEM_DELIVER),
    )(fresh, stepped)
    return fresh[None], next_latent, denoised


def solution(mesh):
    return jax.shard_map(
        functools.partial(body, mesh.shape["patch"]),
        mesh=mesh,
        in_specs=(
            P("cfg", ("groups", "patch"), None),
            P("cfg", ("groups", "patch"), None),
            P(("groups", "cfg"), None, None),
            P(None, None, "head"),
            P(),
            P(),
            P("head", None),
            P(),
            P("cfg", None, ("groups", "patch"), "head"),
            P(("groups", "cfg"), None, None),
            P(),
            P(),
            P(("groups", "patch", "cfg", "head"), None),
            P(("groups", "patch", "cfg", "head"), None),
            P("groups"),
            P(),
            P(),
        ),
        out_specs=(
            P("cfg", None, ("groups", "patch"), "head"),
            P(("groups", "patch", "cfg", "head"), None),
            P(("groups", "patch", "cfg", "head"), None),
        ),
        check_vma=False,
    )
```
